128 devices in a mesh: data: 1, sp: 128 (over z, y, x, core).
Axes of the slice: x: 4, y: 4, z: 4, core: 2. Of those that a mesh axis runs over, the one named last changes fastest.
Arguments:
- latents: bfloat16 [1, 128, 256, 768], P('data', 'sp')
- norms: float32 [4, 4, 768], replicated
- w_qkv: bfloat16 [4, 768, 3, 12, 64], replicated
- w_out: bfloat16 [4, 12, 64, 768], replicated
- w_up: bfloat16 [4, 768, 3072], replicated
- w_down: bfloat16 [4, 3072, 768], replicated
Outputs:
- output: bfloat16 [1, 128, 256, 768], P('data', None, 'sp')
All inputs are finite; a program needn't handle non-finite values.
Results may differ from the reference program's by a relative error of at most 0.0165696.
Values are sent between devices in bfloat16 or wider.
A program may use at most 1 GiB of HBM per device.

```python
import math
import jax
import jax.numpy as jnp
from jax import lax

BATCH = 1
FRAMES = 128
PATCHES = 256
WIDTH = 768
HEADS = 12
BLOCKS = 4
HEAD_DIM = WIDTH // HEADS
HIDDEN = 4 * WIDTH
EPS = 1e-6
SPATIAL = (2, 'btqhe,btkhe->bthqk', 'bthqk,btkhe->btqhe')
TEMPORAL = (1, 'bqshe,bkshe->bshqk', 'bshqk,bkshe->bqshe')


def setup_inputs(seed: int = 0, part: int = 0) -> dict:
    base_key = jax.random.key(seed)
    part_key = jax.random.fold_in(base_key, part)
    time_key, space_key, noise_key = jax.random.split(part_key, 3)
    time_walk = jnp.cumsum(jax.random.normal(time_key, (BATCH, FRAMES, WIDTH), jnp.float32), axis=1) * (1.5 / math.sqrt(FRAMES))
    space_walk = jnp.cumsum(jax.random.normal(space_key, (BATCH, PATCHES, WIDTH), jnp.float32), axis=1) * (1.0 / math.sqrt(PATCHES))
    noise = jax.random.normal(noise_key, (BATCH, FRAMES, PATCHES, WIDTH), jnp.float32)
    latents = (time_walk[:, :, None, :] + space_walk[:, None, :, :] + 0.5 * noise).astype(jnp.bfloat16)
    weight_keys = jax.random.split(jax.random.key(seed + 1), 5)
    norm_base = jnp.array([1.0, 0.0, 1.0, 0.0], jnp.float32)
    norms = norm_base[None, :, None] + 0.3 * jax.random.normal(weight_keys[0], (BLOCKS, 4, WIDTH), jnp.float32)
    qkv_gain = jnp.array([1.2, 1.2, 1.0], jnp.float32)[None, None, :, None, None]
    w_qkv = (jax.random.normal(weight_keys[1], (BLOCKS, WIDTH, 3, HEADS, HEAD_DIM), jnp.float32) * qkv_gain / math.sqrt(WIDTH)).astype(jnp.bfloat16)
    w_out = (jax.random.normal(weight_keys[2], (BLOCKS, HEADS, HEAD_DIM, WIDTH), jnp.float32) / math.sqrt(WIDTH)).astype(jnp.bfloat16)
    w_up = (jax.random.normal(weight_keys[3], (BLOCKS, WIDTH, HIDDEN), jnp.float32) / math.sqrt(WIDTH)).astype(jnp.bfloat16)
    w_down = (jax.random.normal(weight_keys[4], (BLOCKS, HIDDEN, WIDTH), jnp.float32) / math.sqrt(HIDDEN)).astype(jnp.bfloat16)
    return {'latents': latents, 'norms': norms, 'w_qkv': w_qkv, 'w_out': w_out, 'w_up': w_up, 'w_down': w_down}


def layer_norm(tokens, norm_gain, norm_shift):
    tokens_f32 = tokens.astype(jnp.float32)
    row_mean = jnp.mean(tokens_f32, axis=-1, keepdims=True)
    centered = tokens_f32 - row_mean
    variance = jnp.mean(jnp.square(centered), axis=-1, keepdims=True)
    return (centered * lax.rsqrt(variance + EPS) * norm_gain + norm_shift).astype(jnp.bfloat16)


def attention(query_rows, key_rows, value_rows, layout):
    seq_axis, score_form, mix_form = layout
    seq_len = query_rows.shape[seq_axis]
    q_block = math.gcd(seq_len, 64)
    logit_scale = HEAD_DIM ** -0.5
    key_f32 = key_rows.astype(jnp.float32)
    value_f32 = value_rows.astype(jnp.float32)

    def attend_block(block_idx, attn_out):
        q_start = block_idx * q_block
        q_part = lax.dynamic_slice_in_dim(query_rows, q_start, q_block, axis=seq_axis).astype(jnp.float32)
        logits = jnp.einsum(score_form, q_part, key_f32) * logit_scale
        attn_probs = jax.nn.softmax(logits, axis=-1).astype(jnp.bfloat16).astype(jnp.float32)
        block_out = jnp.einsum(mix_form, attn_probs, value_f32).astype(jnp.bfloat16)
        return lax.dynamic_update_slice_in_dim(attn_out, block_out, q_start, axis=seq_axis)

    return lax.fori_loop(0, seq_len // q_block, attend_block, jnp.zeros_like(query_rows))


def project_heads(normed, head_weight):
    return jnp.einsum('btsd,dhe->btshe', normed.astype(jnp.float32), head_weight.astype(jnp.float32)).astype(jnp.bfloat16)


def transformer_block(tokens, norm_rows, qkv_weight, out_weight, up_weight, down_weight, layout):
    normed = layer_norm(tokens, norm_rows[0], norm_rows[1])
    mixed_heads = attention(project_heads(normed, qkv_weight[:, 0]), project_heads(normed, qkv_weight[:, 1]), project_heads(normed, qkv_weight[:, 2]), layout)
    attn_proj = jnp.einsum('btshe,hed->btsd', mixed_heads.astype(jnp.float32), out_weight.astype(jnp.float32))
    residual = (tokens.astype(jnp.float32) + attn_proj).astype(jnp.bfloat16)
    normed_mlp = layer_norm(residual, norm_rows[2], norm_rows[3])
    up_proj = jnp.einsum('btsd,df->btsf', normed_mlp.astype(jnp.float32), up_weight.astype(jnp.float32))
    hidden = jax.nn.gelu(up_proj, approximate=True).astype(jnp.bfloat16)
    down_proj = jnp.einsum('btsf,fd->btsd', hidden.astype(jnp.float32), down_weight.astype(jnp.float32))
    return (residual.astype(jnp.float32) + down_proj).astype(jnp.bfloat16)


def reference(latents, norms, w_qkv, w_out, w_up, w_down):
    tokens = latents
    for layer_idx in range(BLOCKS):
        layout = SPATIAL if layer_idx % 2 == 0 else TEMPORAL
        tokens = transformer_block(tokens, norms[layer_idx], w_qkv[layer_idx], w_out[layer_idx], w_up[layer_idx], w_down[layer_idx], layout)
    return tokens
```

```python
import functools
import jax
import jax.numpy as jnp
from jax import lax
from jax.experimental import pallas as pl
from jax.experimental.pallas import tpu as pltpu
from jax.sharding import PartitionSpec as P

EPS = 1e-6
LOG2E = 1.4426950408889634
GELU_C = 0.7978845608028654
F32 = jnp.float32
BF16 = jnp.bfloat16
ROWS = 32
QKV_ROWS = 768
UP_COLS = 512


def matmul(a, b, dims):
    return lax.dot_general(a, b, (dims, ((), ())), preferred_element_type=F32)


def normalize(u, gain, shift):
    mean = jnp.mean(u, axis=-1, keepdims=True)
    centered = u - mean
    var = jnp.mean(jnp.square(centered), axis=-1, keepdims=True)
    return (centered * lax.rsqrt(var + EPS) * gain + shift).astype(BF16)


def softmax_t(scores, scale):
    top = jnp.max(scores, axis=0, keepdims=True)
    e = jnp.exp2((scores - top) * (scale * LOG2E))
    return (e * (1.0 / jnp.sum(e, axis=0, keepdims=True))).astype(BF16)


def gelu(x):
    return 0.5 * x * (1.0 + jnp.tanh(GELU_C * (x + 0.044715 * (x * x * x))))


def block(u_ref, norm, wqkv, wout, wup, wdown, a_ref, qkv_ref, o_ref, h_ref, hid_ref, s_ref, p_ref, perm_ref, heads, segments, wait, emit):
    rows, width = u_ref.shape
    head_dim = width // heads
    hidden = hid_ref.shape[1]
    span = rows // segments
    wait(0)
    for r in range(0, rows, ROWS):
        a_ref[r:r + ROWS] = normalize(u_ref[r:r + ROWS].astype(F32), norm[0:1], norm[1:2])
    if segments > 1:
        a_ref[...] = matmul(perm_ref[...], a_ref[...], ((1,), (0,))).astype(BF16)
    wait(1)
    for r in range(0, 3 * width, QKV_ROWS):
        qkv_ref[r:r + QKV_ROWS] = matmul(wqkv[r:r + QKV_ROWS], a_ref[...], ((1,), (1,))).astype(BF16)
    units = [(h, slice(s * span, (s + 1) * span)) for h in range(heads) for s in range(segments)]
    for i, (h, cols) in enumerate(units):
        q = qkv_ref[h * head_dim:(h + 1) * head_dim, cols]
        k = qkv_ref[width + h * head_dim:width + (h + 1) * head_dim, cols]
        s_ref[i * span:(i + 1) * span, :span] = matmul(k, q, ((0,), (0,)))
    for i, (h, cols) in enumerate(units):
        p_ref[i * span:(i + 1) * span, :span] = softmax_t(s_ref[i * span:(i + 1) * span, :span], head_dim ** -0.5)
    for i, (h, cols) in enumerate(units):
        v = qkv_ref[2 * width + h * head_dim:2 * width + (h + 1) * head_dim, cols]
        o_ref[h * head_dim:(h + 1) * head_dim, cols] = matmul(v, p_ref[i * span:(i + 1) * span, :span], ((1,), (0,))).astype(BF16)
    if segments > 1:
        o_ref[...] = matmul(o_ref[...], perm_ref[...], ((1,), (0,))).astype(BF16)
    wait(2)
    h_ref[...] = (u_ref[...].astype(F32) + matmul(o_ref[...], wout[...], ((0,), (0,)))).astype(BF16)
    for r in range(0, rows, ROWS):
        a_ref[r:r + ROWS] = normalize(h_ref[r:r + ROWS].astype(F32), norm[2:3], norm[3:4])
    wait(3)
    for c in range(0, hidden, UP_COLS):
        hid_ref[:, c:c + UP_COLS] = gelu(matmul(a_ref[...], wup[:, c:c + UP_COLS], ((1,), (0,)))).astype(BF16)
    wait(4)
    emit((h_ref[...].astype(F32) + matmul(hid_ref[...], wdown[...], ((1,), (0,)))).astype(BF16))


def exchange(peers, send, recv, send_sem, recv_sem, first):
    me = lax.axis_index('sp')

    def give(k, carry):
        peer = lax.rem(me + k, peers)
        pltpu.make_async_remote_copy(src_ref=send.at[peer], dst_ref=recv.at[me], send_sem=send_sem, recv_sem=recv_sem, device_id={'sp': peer}, device_id_type=pl.DeviceIdType.MESH).start()
        return carry

    if first:
        pl.semaphore_wait(pltpu.get_barrier_semaphore(), peers - 1)
    lax.fori_loop(1, peers, give, 0)
    recv[pl.ds(me, 1)] = send[pl.ds(me, 1)]


def exchanged(peers, send, recv, send_sem, recv_sem):
    other = lax.rem(lax.axis_index('sp') + 1, peers)
    return pltpu.make_async_remote_copy(src_ref=send.at[pl.ds(0, peers - 1)], dst_ref=recv.at[pl.ds(0, peers - 1)], send_sem=send_sem, recv_sem=recv_sem, device_id={'sp': other}, device_id_type=pl.DeviceIdType.MESH)


def stack_kernel(heads, x_ref, norm_ref, wqkv_hbm, wout_hbm, wup_hbm, wdown_hbm, y_ref, wqkv, wout, wup, wdown, a_ref, qkv_ref, o_ref, h_ref, hid_ref, s_ref, p_ref, perm_ref, u_ref, send, recv, weight_sem, send_sem, recv_sem):
    layers = wqkv_hbm.shape[0]
    peers = send.shape[1]
    rows, width = u_ref.shape
    held = rows // peers
    me = lax.axis_index('sp')

    def load(layer, part):
        hbm, vmem = ((wqkv_hbm, wqkv), (wout_hbm, wout), (wup_hbm, wup), (wdown_hbm, wdown))[part]
        return pltpu.make_async_copy(hbm.at[layer], vmem.at[layer % 2], weight_sem.at[layer % 2, part])

    for layer in range(2):
        for part in range(4):
            load(layer, part).start()

    def greet(k, carry):
        pl.semaphore_signal(pltpu.get_barrier_semaphore(), inc=1, device_id={'sp': lax.rem(me + k, peers)}, device_id_type=pl.DeviceIdType.MESH)
        return carry

    lax.fori_loop(1, peers, greet, 0)
    row = lax.broadcasted_iota(jnp.int32, (rows, rows), 0)
    col = lax.broadcasted_iota(jnp.int32, (rows, rows), 1)
    perm_ref[...] = jnp.where(col == held * (row % peers) + row // peers, 1.0, 0.0).astype(BF16)

    for layer in range(layers):
        slot = layer % 2

        def wait(stage):
            if stage > 0:
                load(layer, stage - 1).wait()
            elif layer > 0:
                exchanged(peers, send.at[layer - 1], recv.at[layer - 1], send_sem.at[layer - 1], recv_sem.at[layer - 1]).wait_recv()
                u_ref[...] = recv[layer - 1].reshape(rows, width)

        def emit(z):
            z = z.reshape(peers, held, width)
            if layer == layers - 1:
                y_ref[...] = z
            else:
                send[layer] = z
                exchange(peers, send.at[layer], recv.at[layer], send_sem.at[layer], recv_sem.at[layer], layer == 0)

        block(u_ref if layer else x_ref, norm_ref.at[layer], wqkv.at[slot], wout.at[slot], wup.at[slot], wdown.at[slot], a_ref, qkv_ref, o_ref, h_ref, hid_ref, s_ref, p_ref, perm_ref, heads, held if layer % 2 else 1, wait, emit)
        if layer + 2 < layers:
            for part in range(4):
                load(layer + 2, part).start()
    for layer in range(layers - 1):
        exchanged(peers, send.at[layer], recv.at[layer], send_sem.at[layer], recv_sem.at[layer]).wait_send()


def solution(mesh):
    peers = mesh.shape['sp']

    def local_stack(latents, norms, w_qkv, w_out, w_up, w_down):
        layers, width, _, heads, head_dim = w_qkv.shape
        hidden = w_up.shape[2]
        rows = latents.shape[2]
        held = rows // peers
        vmem = pl.BlockSpec(memory_space=pltpu.VMEM)
        hbm = pl.BlockSpec(memory_space=pl.ANY)
        y = pl.pallas_call(
            functools.partial(stack_kernel, heads),
            out_shape=jax.ShapeDtypeStruct((peers, held, width), BF16),
            in_specs=[vmem, vmem, hbm, hbm, hbm, hbm],
            out_specs=vmem,
            scratch_shapes=[
                pltpu.VMEM((2, 3 * width, width), BF16),
                pltpu.VMEM((2, width, width), BF16),
                pltpu.VMEM((2, width, hidden), BF16),
                pltpu.VMEM((2, hidden, width), BF16),
                pltpu.VMEM((rows, width), BF16),
                pltpu.VMEM((3 * width, rows), BF16),
                pltpu.VMEM((width, rows), BF16),
                pltpu.VMEM((rows, width), BF16),
                pltpu.VMEM((rows, hidden), BF16),
                pltpu.VMEM((heads * rows, rows), F32),
                pltpu.VMEM((heads * rows, rows), BF16),
                pltpu.VMEM((rows, rows), BF16),
                pltpu.VMEM((rows, width), BF16),
                pltpu.VMEM((layers - 1, peers, held, width), BF16),
                pltpu.VMEM((layers - 1, peers, held, width), BF16),
                pltpu.SemaphoreType.DMA((2, 4)),
                pltpu.SemaphoreType.DMA((layers - 1,)),
                pltpu.SemaphoreType.DMA((layers - 1,)),
            ],
            compiler_params=pltpu.CompilerParams(collective_id=0, has_side_effects=True, vmem_limit_bytes=62 * 2 ** 20),
            name='stack',
        )(
            latents.reshape(rows, width),
            norms,
            w_qkv.transpose(0, 2, 3, 4, 1).reshape(layers, 3 * width, width),
            w_out.reshape(layers, width, width),
            w_up,
            w_down,
        )
        return y.reshape(1, peers, held, width)

    whole = P()
    return jax.shard_map(local_stack, mesh=mesh, in_specs=(P('data', 'sp', None, None), whole, whole, whole, whole, whole), out_specs=P('data', None, 'sp', None), check_vma=False)
```
